8 devices in a mesh: tp: 2 (over z, y), dp: 4 (over x, core).
Axes of the slice: x: 2, y: 2, z: 1, core: 2. Of those that a mesh axis runs over, the one named last changes fastest.
Arguments:
- h_teacher: bfloat16 [16384, 3584], P('dp')
- h_student: bfloat16 [16384, 1536], P('dp')
- w_teacher: bfloat16 [3584, 4096], P(None, 'tp')
- w_student: bfloat16 [1536, 4096], P(None, 'tp')
Outputs:
- output 1: float32 [], replicated
- output 2: float32 [16384, 1536], P('dp')
- output 3: float32 [1536, 4096], P(None, 'tp')
All inputs are finite; a program needn't handle non-finite values.
Results may differ from the reference program's by a relative error of at most 0.001.
Values sent between devices are 32-bit elements.
A program may use at most 1 GiB of HBM per device.

```python
import jax
import jax.numpy as jnp
from jax import lax

TOKENS = 16384
VOCAB = 4096
D_TEACHER = 3584
D_STUDENT = 1536
ROW_BLOCK = 256


def setup_inputs(seed: int = 0) -> dict:
    root_key = jax.random.key(seed)
    key_ht, key_hs, key_wt, key_ws = jax.random.split(root_key, 4)
    h_teacher = jax.random.normal(key_ht, (TOKENS, D_TEACHER), jnp.float32)
    h_student = jax.random.normal(key_hs, (TOKENS, D_STUDENT), jnp.float32)
    w_teacher = jax.random.normal(key_wt, (D_TEACHER, VOCAB), jnp.float32) * (2.0 * D_TEACHER ** -0.5)
    w_student = jax.random.normal(key_ws, (D_STUDENT, VOCAB), jnp.float32) * (1.5 * D_STUDENT ** -0.5)
    return {
        "h_teacher": h_teacher.astype(jnp.bfloat16),
        "h_student": h_student.astype(jnp.bfloat16),
        "w_teacher": w_teacher.astype(jnp.bfloat16),
        "w_student": w_student.astype(jnp.bfloat16),
    }


def log_probs(logits):
    row_max = jnp.max(logits, axis=1, keepdims=True)
    shifted = logits - row_max
    exp_vals = jnp.exp(shifted)
    row_sum = jnp.sum(exp_vals, axis=1, keepdims=True)
    return exp_vals / row_sum, shifted - jnp.log(row_sum)


def reference(h_teacher, h_student, w_teacher, w_student):
    num_blocks = TOKENS // ROW_BLOCK
    ht_blocks = h_teacher.reshape(num_blocks, ROW_BLOCK, D_TEACHER)
    hs_blocks = h_student.reshape(num_blocks, ROW_BLOCK, D_STUDENT)

    def scan_step(dw_acc, block_pair):
        ht_block, hs_block = block_pair
        prob_t, logp_t = log_probs(jnp.dot(ht_block, w_teacher, preferred_element_type=jnp.float32))
        prob_s, logp_s = log_probs(jnp.dot(hs_block, w_student, preferred_element_type=jnp.float32))
        kl_rows = jnp.sum(prob_t * (logp_t - logp_s), axis=1)
        dz_student = ((prob_s - prob_t) / TOKENS).astype(jnp.bfloat16)
        dh_block = jnp.dot(dz_student, w_student.T, preferred_element_type=jnp.float32)
        dw_acc = dw_acc + jnp.dot(hs_block.T, dz_student, preferred_element_type=jnp.float32)
        return dw_acc, (kl_rows, dh_block)

    dw_start = jnp.zeros((D_STUDENT, VOCAB), jnp.float32)
    dw_student, (kl_rows, dh_blocks) = lax.scan(scan_step, dw_start, (ht_blocks, hs_blocks))
    kl_loss = jnp.sum(kl_rows) / TOKENS
    return kl_loss, dh_blocks.reshape(TOKENS, D_STUDENT), dw_student
```

```python
import functools

import jax
import jax.numpy as jnp
from jax import lax
from jax.experimental import pallas as pl
from jax.experimental.pallas import tpu as pltpu
from jax.sharding import PartitionSpec as P

F32 = jnp.float32
BF16 = jnp.bfloat16
VMEM_LIMIT = 67043328
ONCE = pl.Buffered(buffer_count=1)


def params():
    return pltpu.CompilerParams(vmem_limit_bytes=VMEM_LIMIT, dimension_semantics=("arbitrary",))


def cost(flops, nbytes):
    return pl.CostEstimate(flops=int(flops), bytes_accessed=int(nbytes), transcendentals=0)


def lane_fold(x, op):
    acc = x[:, 0:128]
    for j in range(1, x.shape[1] // 128):
        acc = op(acc, x[:, 128 * j:128 * (j + 1)])
    return acc


def logits_body(rows, tile, ht_ref, hs_ref, wt_ref, ws_ref, *rest):
    et_ref, es_ref, stat_ref = rest[-3:]
    block, cols = et_ref.shape
    for r in range(0, block, rows):
        sl = pl.ds(r, rows)
        ht = ht_ref[sl, :]
        hs = hs_ref[sl, :]
        mt = jnp.full((rows, 128), -jnp.inf, F32)
        ms = mt
        for c in range(0, cols, tile):
            zt = jnp.dot(ht, wt_ref[:, c:c + tile], preferred_element_type=F32)
            et_ref[sl, c:c + tile] = zt
            mt = jnp.maximum(mt, lane_fold(zt, jnp.maximum))
            zs = jnp.dot(hs, ws_ref[:, c:c + tile], preferred_element_type=F32)
            es_ref[sl, c:c + tile] = zs
            ms = jnp.maximum(ms, lane_fold(zs, jnp.maximum))
        mt = jnp.max(mt, axis=1, keepdims=True)
        ms = jnp.max(ms, axis=1, keepdims=True)
        st = jnp.zeros((rows, 128), F32)
        ss = st
        dd = st
        for c in range(0, cols, 128):
            xt = et_ref[sl, c:c + 128] - mt
            xs = es_ref[sl, c:c + 128] - ms
            pt = jnp.exp(xt)
            ps = jnp.exp(xs)
            et_ref[sl, c:c + 128] = pt
            es_ref[sl, c:c + 128] = ps
            st = st + pt
            ss = ss + ps
            dd = dd + pt * (xt - xs)
        vals = (mt, jnp.sum(st, axis=1, keepdims=True), ms, jnp.sum(ss, axis=1, keepdims=True),
                jnp.sum(dd, axis=1, keepdims=True))
        lane = lax.broadcasted_iota(jnp.int32, (rows, 128), 1)
        packed = jnp.zeros((rows, 128), F32)
        for i, v in enumerate(vals):
            packed = jnp.where(lane == i, v, packed)
        stat_ref[:, r:r + rows] = jnp.transpose(packed)[0:8, :]


def logits_part(ht, hs, wt, ws, start, count, prev, block=512, rows=256, tile=512):
    tokens, kt = ht.shape
    ks, cols = ws.shape
    first = start // block
    tok = lambda i: (i + first, 0)
    fixed = lambda i: (0, 0)
    in_specs = [pl.BlockSpec((block, kt), tok), pl.BlockSpec((block, ks), tok),
                pl.BlockSpec((kt, cols), fixed, pipeline_mode=ONCE),
                pl.BlockSpec((ks, cols), fixed, pipeline_mode=ONCE)]
    args = [ht, hs, wt, ws]
    alias = {}
    if prev is not None:
        in_specs += [pl.BlockSpec(memory_space=pl.ANY)] * 2
        args += list(prev)
        alias = {4: 0, 5: 1}
    return pl.pallas_call(
        functools.partial(logits_body, rows, tile),
        grid=(count // block,),
        in_specs=in_specs,
        out_specs=[pl.BlockSpec((block, cols), tok), pl.BlockSpec((block, cols), tok),
                   pl.BlockSpec((8, block), lambda i: (0, i))],
        out_shape=[jax.ShapeDtypeStruct((tokens, cols), F32), jax.ShapeDtypeStruct((tokens, cols), F32),
                   jax.ShapeDtypeStruct((8, count), F32)],
        input_output_aliases=alias,
        compiler_params=params(),
        cost_estimate=cost(2 * count * cols * (kt + ks), 2 * cols * (kt + ks) + count * (2 * (kt + ks) + 8 * cols)),
        name="logits",
    )(*args)


def grads_body(hs_ref, ws_ref, et_ref, es_ref, coef_ref, dh_ref, dw_hbm, acc_ref, sem):
    i = pl.program_id(0)
    coef = jnp.transpose(coef_ref[...])
    dz = (es_ref[...] * coef[:, 1:2] - et_ref[...] * coef[:, 0:1]).astype(BF16)
    dh_ref[...] = lax.dot_general(dz, ws_ref[...], (((1,), (1,)), ((), ())), preferred_element_type=F32)
    part = lax.dot_general(hs_ref[...], dz, (((0,), (0,)), ((), ())), preferred_element_type=F32)
    ks = hs_ref.shape[1]
    block = hs_ref.shape[0]

    @pl.when(i == 0)
    def _():
        acc_ref[0:ks, :] = part
        acc_ref[ks:ks + 8, :] = jnp.zeros((8, acc_ref.shape[1]), F32)

    @pl.when(i > 0)
    def _():
        acc_ref[0:ks, :] += part

    acc_ref[ks:ks + 8, 0:block] += coef_ref[...]

    @pl.when(i == pl.num_programs(0) - 1)
    def _():
        copy = pltpu.make_async_copy(acc_ref, dw_hbm, sem)
        copy.start()
        copy.wait()


def grads_part(hs, ws, et, es, coef, block=512):
    tokens, ks = hs.shape
    cols = ws.shape[1]
    tok = lambda i: (i, 0)
    return pl.pallas_call(
        grads_body,
        grid=(tokens // block,),
        in_specs=[pl.BlockSpec((block, ks), tok), pl.BlockSpec((ks, cols), lambda i: (0, 0), pipeline_mode=ONCE),
                  pl.BlockSpec((block, cols), tok), pl.BlockSpec((block, cols), tok),
                  pl.BlockSpec((8, block), lambda i: (0, i))],
        out_specs=[pl.BlockSpec((block, ks), tok), pl.BlockSpec(memory_space=pl.ANY)],
        out_shape=[jax.ShapeDtypeStruct((tokens, ks), F32), jax.ShapeDtypeStruct((ks + 8, cols), F32)],
        scratch_shapes=[pltpu.VMEM((ks + 8, cols), F32), pltpu.SemaphoreType.DMA],
        compiler_params=params(),
        cost_estimate=cost(4 * tokens * cols * ks, 2 * ks * cols + tokens * (6 * ks + 8 * cols) + 4 * ks * cols),
        name="grads",
    )(hs, ws, et, es, coef)


def other_body(npieces, rows, ht_ref, hs_ref, coef_ref, *rest):
    pieces = rest[:npieces]
    dh_in_ref, dh_ref, wt_ref, ws_ref = rest[npieces:]
    kt = ht_ref.shape[1]

    @pl.when(pl.program_id(0) == 0)
    def _():
        at = 0
        for p in pieces:
            w = p.shape[1]
            wt_ref[:, at:at + w] = p[0:kt, :].astype(BF16)
            ws_ref[:, at:at + w] = p[kt:, :].astype(BF16)
            at += w

    for r in range(0, ht_ref.shape[0], rows):
        sl = pl.ds(r, rows)
        coef = jnp.transpose(coef_ref[:, r:r + rows])
        zt = jnp.dot(ht_ref[sl, :], wt_ref[...], preferred_element_type=F32)
        zs = jnp.dot(hs_ref[sl, :], ws_ref[...], preferred_element_type=F32)
        pt = jnp.exp(zt - coef[:, 2:3]) * coef[:, 3:4]
        ps = jnp.exp(zs - coef[:, 4:5]) * coef[:, 5:6]
        dz = (ps - pt).astype(BF16)
        dh_ref[sl, :] = dh_in_ref[sl, :] + lax.dot_general(
            dz, ws_ref[...], (((1,), (1,)), ((), ())), preferred_element_type=F32)


def other_part(ht, hs, coef, pieces, dh, block=512, rows=256):
    tokens, kt = ht.shape
    ks = hs.shape[1]
    cols = sum(p.shape[1] for p in pieces)
    tok = lambda i: (i, 0)
    fixed = lambda i: (0, 0)
    n = len(pieces)
    return pl.pallas_call(
        functools.partial(other_body, n, rows),
        grid=(tokens // block,),
        in_specs=[pl.BlockSpec((block, kt), tok), pl.BlockSpec((block, ks), tok), pl.BlockSpec((8, block), lambda i: (0, i))]
        + [pl.BlockSpec(p.shape, fixed, pipeline_mode=ONCE) for p in pieces]
        + [pl.BlockSpec((block, ks), tok)],
        out_specs=pl.BlockSpec((block, ks), tok),
        out_shape=jax.ShapeDtypeStruct((tokens, ks), F32),
        scratch_shapes=[pltpu.VMEM((kt, cols), BF16), pltpu.VMEM((ks, cols), BF16)],
        input_output_aliases={3 + n: 0},
        compiler_params=params(),
        cost_estimate=cost(2 * tokens * cols * (kt + 2 * ks), 4 * cols * (kt + ks) + tokens * (2 * kt + 10 * ks)),
        name="other",
    )(ht, hs, coef, *pieces, dh)


def solution(mesh):
    dp_size = mesh.shape["dp"]
    swap_tp = [(0, 1), (1, 0)]
    swap_x = [(i, i ^ 2) for i in range(dp_size)]
    swap_core = [(i, i ^ 1) for i in range(dp_size)]

    def local_step(h_teacher, h_student, w_teacher, w_student):
        tokens = h_teacher.shape[0]
        tok_total = tokens * dp_size
        half = tokens // 2
        tp = lax.axis_index("tp")
        dp = lax.axis_index("dp")

        def piece(start, width):
            return jnp.concatenate([lax.dynamic_slice_in_dim(w_teacher, start, width, 1),
                                    lax.dynamic_slice_in_dim(w_student, start, width, 1)], axis=0).astype(F32)

        def over(axis, perm, x):
            return lax.ppermute(x, axis, perm)

        y0 = over("tp", swap_tp, piece(128 * dp, 128))
        y1 = over("tp", swap_tp, piece(512 + 128 * dp, 128))
        et, es, stat_a = logits_part(h_teacher, h_student, w_teacher, w_student, 0, half, None)
        x0 = over("dp", swap_x, y0)
        et, es, stat_b = logits_part(h_teacher, h_student, w_teacher, w_student, half, half, (et, es))
        stat = jnp.concatenate([stat_a, stat_b], axis=1)
        stat_other = over("tp", swap_tp, stat)
        x1 = over("dp", swap_x, y1)

        first = jnp.where(tp == 0, stat, stat_other)
        second = jnp.where(tp == 0, stat_other, stat)
        max_t = jnp.maximum(first[0], second[0])
        max_s = jnp.maximum(first[2], second[2])
        scale_t1, scale_t2 = jnp.exp(first[0] - max_t), jnp.exp(second[0] - max_t)
        scale_s1, scale_s2 = jnp.exp(first[2] - max_s), jnp.exp(second[2] - max_s)
        sum_t = first[1] * scale_t1 + second[1] * scale_t2
        sum_s = first[3] * scale_s1 + second[3] * scale_s2
        inv_t = (1.0 / sum_t) / tok_total
        inv_s = (1.0 / sum_s) / tok_total
        own_t = jnp.exp(stat[0] - max_t) * inv_t
        own_s = jnp.exp(stat[2] - max_s) * inv_s
        num = (scale_t1 * (first[4] + first[1] * ((first[0] - max_t) - (first[2] - max_s)))
               + scale_t2 * (second[4] + second[1] * ((second[0] - max_t) - (second[2] - max_s))))
        kl = num / sum_t - (jnp.log(sum_t) - jnp.log(sum_s))
        coef = jnp.stack([own_t, own_s, max_t, inv_t, max_s, inv_s, kl, jnp.zeros_like(kl)])

        core = dp % 2
        p2, p3, coef = lax.optimization_barrier((piece(1024 + 256 * core, 256), piece(1536 + 256 * core, 256), coef))
        y2 = over("tp", swap_tp, p2)
        y3 = over("tp", swap_tp, p3)
        dh, dw = grads_part(h_student, w_student, et, es, coef)
        dw = lax.psum(dw, "dp")
        cy0 = over("dp", swap_core, y0)
        cx0 = over("dp", swap_core, x0)
        cy1 = over("dp", swap_core, y1)
        cx1 = over("dp", swap_core, x1)
        cy2 = over("dp", swap_core, y2)
        cy3 = over("dp", swap_core, y3)
        for pieces in ((y0, x0, cy0, cx0), (y1, x1, cy1, cx1),
                             (y2, cy2), (y3, cy3)):
            dh = other_part(h_teacher, h_student, coef, pieces, dh)
        depth = h_student.shape[1]
        kl_loss = jnp.sum(dw[depth + 6]) / tok_total
        return kl_loss, dh, dw[0:depth]

    return jax.shard_map(
        local_step, mesh=mesh,
        in_specs=(P("dp", None), P("dp", None), P(None, "tp"), P(None, "tp")),
        out_specs=(P(), P("dp", None), P(None, "tp")),
        check_vma=False)
```

```python
import functools

import jax
import jax.numpy as jnp
from jax import lax
from jax.experimental import pallas as pl
from jax.experimental.pallas import tpu as pltpu
from jax.sharding import PartitionSpec as P

F32 = jnp.float32
BF16 = jnp.bfloat16
VMEM_LIMIT = 67043328
ONCE = pl.Buffered(buffer_count=1)


def params():
    return pltpu.CompilerParams(vmem_limit_bytes=VMEM_LIMIT, dimension_semantics=("arbitrary",))


def cost(flops, nbytes):
    return pl.CostEstimate(flops=int(flops), bytes_accessed=int(nbytes), transcendentals=0)


def lane_fold(x, op):
    acc = x[:, 0:128]
    for j in range(1, x.shape[1] // 128):
        acc = op(acc, x[:, 128 * j:128 * (j + 1)])
    return acc


def logits_body(tile, ht_ref, hs_ref, wt_ref, ws_ref, *rest):
    et_ref, es_ref, stat_ref = rest[-3:]
    rows, cols = et_ref.shape
    low = jnp.full((rows, 128), -jnp.inf, F32)

    def products(c, carry):
        mt, ms = carry
        at = pl.ds(pl.multiple_of(c * tile, tile), tile)
        zt = jnp.dot(ht_ref[...], wt_ref[:, at], preferred_element_type=F32)
        et_ref[:, at] = zt
        mt = jnp.maximum(mt, lane_fold(zt, jnp.maximum))
        zs = jnp.dot(hs_ref[...], ws_ref[:, at], preferred_element_type=F32)
        es_ref[:, at] = zs
        return mt, jnp.maximum(ms, lane_fold(zs, jnp.maximum))

    mt, ms = lax.fori_loop(0, cols // tile, products, (low, low))
    mt = jnp.max(mt, axis=1, keepdims=True)
    ms = jnp.max(ms, axis=1, keepdims=True)
    zero = jnp.zeros((rows, 128), F32)
    step = 256

    def exps(c, carry):
        st, ss, dd = carry
        at = pl.ds(pl.multiple_of(c * step, step), step)
        xt = et_ref[:, at] - mt
        xs = es_ref[:, at] - ms
        pt = jnp.exp(xt)
        ps = jnp.exp(xs)
        et_ref[:, at] = pt
        es_ref[:, at] = ps
        return st + lane_fold(pt, jnp.add), ss + lane_fold(ps, jnp.add), dd + lane_fold(pt * (xt - xs), jnp.add)

    st, ss, dd = lax.fori_loop(0, cols // step, exps, (zero, zero, zero))
    vals = (mt, jnp.sum(st, axis=1, keepdims=True), ms, jnp.sum(ss, axis=1, keepdims=True),
            jnp.sum(dd, axis=1, keepdims=True))
    lane = lax.broadcasted_iota(jnp.int32, (rows, 128), 1)
    packed = zero
    for i, v in enumerate(vals):
        packed = jnp.where(lane == i, v, packed)
    stat_ref[...] = jnp.transpose(packed)[0:8, :]


def logits_part(ht, hs, wt, ws, start, count, prev, block=512, tile=512):
    tokens, kt = ht.shape
    ks, cols = ws.shape
    first = start // block
    tok = lambda i: (i + first, 0)
    fixed = lambda i: (0, 0)
    in_specs = [pl.BlockSpec((block, kt), tok), pl.BlockSpec((block, ks), tok),
                pl.BlockSpec((kt, cols), fixed, pipeline_mode=ONCE),
                pl.BlockSpec((ks, cols), fixed, pipeline_mode=ONCE)]
    args = [ht, hs, wt, ws]
    alias = {}
    if prev is not None:
        in_specs += [pl.BlockSpec(memory_space=pl.ANY)] * 2
        args += list(prev)
        alias = {4: 0, 5: 1}
    return pl.pallas_call(
        functools.partial(logits_body, tile),
        grid=(count // block,),
        in_specs=in_specs,
        out_specs=[pl.BlockSpec((block, cols), tok), pl.BlockSpec((block, cols), tok),
                   pl.BlockSpec((8, block), lambda i: (0, i))],
        out_shape=[jax.ShapeDtypeStruct((tokens, cols), F32), jax.ShapeDtypeStruct((tokens, cols), F32),
                   jax.ShapeDtypeStruct((8, count), F32)],
        input_output_aliases=alias,
        compiler_params=params(),
        cost_estimate=cost(2 * count * cols * (kt + ks), 2 * cols * (kt + ks) + count * (2 * (kt + ks) + 8 * cols)),
        name="logits",
    )(*args)


def grads_body(core_ref, hs_ref, ws_ref, et_ref, es_ref, coef_ref, dh_ref, mine_hbm, theirs_hbm, acc_ref, sem):
    i = pl.program_id(0)
    core = core_ref[0]
    block, ks = hs_ref.shape
    width = acc_ref.shape[2]

    @pl.when(i == 0)
    def _():
        acc_ref[...] = jnp.zeros(acc_ref.shape, F32)

    coef = jnp.transpose(coef_ref[...])
    dz = (es_ref[...] * coef[:, 1:2] - et_ref[...] * coef[:, 0:1]).astype(BF16)
    dh_ref[...] = lax.dot_general(dz, ws_ref[...], (((1,), (1,)), ((), ())), preferred_element_type=F32)
    hs_t = jnp.transpose(hs_ref[...])
    for c in range(0, 2 * width, 512):
        half, at = c // width, c % width
        acc_ref[half, 0:ks, at:at + 512] += jnp.dot(hs_t, dz[:, c:c + 512], preferred_element_type=F32)
    for half in range(2):
        acc_ref[half, ks:ks + 8, 0:block] += coef_ref[...]

    @pl.when(i == pl.num_programs(0) - 1)
    def _():
        first = pltpu.make_async_copy(acc_ref.at[1 - core], theirs_hbm, sem.at[0])
        second = pltpu.make_async_copy(acc_ref.at[core], mine_hbm, sem.at[1])
        first.start()
        second.start()
        first.wait()
        second.wait()


def grads_part(core, hs, ws, et, es, coef, block=512):
    tokens, ks = hs.shape
    cols = ws.shape[1]
    tok = lambda i, c: (i, 0)
    half = jax.ShapeDtypeStruct((ks + 8, cols // 2), F32)
    return pl.pallas_call(
        grads_body,
        grid_spec=pltpu.PrefetchScalarGridSpec(
            num_scalar_prefetch=1,
            grid=(tokens // block,),
            in_specs=[pl.BlockSpec((block, ks), tok), pl.BlockSpec((ks, cols), lambda i, c: (0, 0), pipeline_mode=ONCE),
                      pl.BlockSpec((block, cols), tok), pl.BlockSpec((block, cols), tok),
                      pl.BlockSpec((8, block), lambda i, c: (0, i))],
            out_specs=[pl.BlockSpec((block, ks), tok), pl.BlockSpec(memory_space=pl.ANY),
                       pl.BlockSpec(memory_space=pl.ANY)],
            scratch_shapes=[pltpu.VMEM((2, ks + 8, cols // 2), F32), pltpu.SemaphoreType.DMA((2,))]),
        out_shape=[jax.ShapeDtypeStruct((tokens, ks), F32), half, half],
        compiler_params=params(),
        cost_estimate=cost(4 * tokens * cols * ks, 2 * ks * cols + tokens * (6 * ks + 8 * cols) + 4 * ks * cols),
        name="grads",
    )(core, hs, ws, et, es, coef)


def other_body(kinds, rows, ht_ref, hs_ref, coef_ref, *rest):
    pieces = rest[:len(kinds)]
    dh_in_ref, dh_ref, wt_ref, ws_ref = rest[len(kinds):]
    kt = ht_ref.shape[1]

    @pl.when(pl.program_id(0) == 0)
    def _():
        at_t = at_s = 0
        for kind, p in zip(kinds, pieces):
            w = p.shape[1]
            if "t" in kind:
                wt_ref[:, at_t:at_t + w] = p[0:kt, :].astype(BF16)
                at_t += w
            if "s" in kind:
                ws_ref[:, at_s:at_s + w] = p[p.shape[0] - ws_ref.shape[0]:, :].astype(BF16)
                at_s += w

    for r in range(0, ht_ref.shape[0], rows):
        sl = pl.ds(r, rows)
        coef = jnp.transpose(coef_ref[:, r:r + rows])
        zt = jnp.dot(ht_ref[sl, :], wt_ref[...], preferred_element_type=F32)
        zs = jnp.dot(hs_ref[sl, :], ws_ref[...], preferred_element_type=F32)
        pt = jnp.exp(zt - coef[:, 2:3]) * coef[:, 3:4]
        ps = jnp.exp(zs - coef[:, 4:5]) * coef[:, 5:6]
        dz = (ps - pt).astype(BF16)
        dh_ref[sl, :] = dh_in_ref[sl, :] + lax.dot_general(
            dz, ws_ref[...], (((1,), (1,)), ((), ())), preferred_element_type=F32)


def other_part(ht, hs, coef, pieces, dh, block=512, rows=512):
    tokens, kt = ht.shape
    ks = hs.shape[1]
    kinds = tuple(k for k, _ in pieces)
    arrays = [p for _, p in pieces]
    cols = sum(p.shape[1] for k, p in pieces if "t" in k)
    tok = lambda i: (i, 0)
    fixed = lambda i: (0, 0)
    n = len(pieces)
    return pl.pallas_call(
        functools.partial(other_body, kinds, rows),
        grid=(tokens // block,),
        in_specs=[pl.BlockSpec((block, kt), tok), pl.BlockSpec((block, ks), tok), pl.BlockSpec((8, block), lambda i: (0, i))]
        + [pl.BlockSpec(p.shape, fixed, pipeline_mode=ONCE) for p in arrays]
        + [pl.BlockSpec((block, ks), tok)],
        out_specs=pl.BlockSpec((block, ks), tok),
        out_shape=jax.ShapeDtypeStruct((tokens, ks), F32),
        scratch_shapes=[pltpu.VMEM((kt, cols), BF16), pltpu.VMEM((ks, cols), BF16)],
        input_output_aliases={3 + n: 0},
        compiler_params=params(),
        cost_estimate=cost(2 * tokens * cols * (kt + 2 * ks), 4 * cols * (kt + ks) + tokens * (2 * kt + 10 * ks)),
        name="other",
    )(ht, hs, coef, *arrays, dh)


def cast_part(weights, blocks):
    depth = sum(w.shape[0] for w in weights)

    def body(at_ref, *refs):
        row = 0
        for ref in refs[:-1]:
            refs[-1][row:row + ref.shape[0], :] = ref[...].astype(F32)
            row += ref.shape[0]

    return pl.pallas_call(
        body,
        grid_spec=pltpu.PrefetchScalarGridSpec(
            num_scalar_prefetch=1,
            grid=(len(blocks),),
            in_specs=[pl.BlockSpec((w.shape[0], 128), lambda i, at: (0, at[i])) for w in weights],
            out_specs=pl.BlockSpec((depth, 128), lambda i, at: (0, i))),
        out_shape=jax.ShapeDtypeStruct((depth, 128 * len(blocks)), F32),
        compiler_params=params(),
        cost_estimate=cost(128 * depth, 768 * depth * len(blocks)),
        name="cast",
    )(jnp.stack(blocks).astype(jnp.int32), *weights)


def total_part(half, a, b, row, rows, shape, prev=None, block=384):
    width = shape[1] // 2

    def body(half_ref, a_ref, b_ref, *rest):
        rest[-1][...] = a_ref[...] + b_ref[...]

    here = lambda i, h: (i, 0)
    return pl.pallas_call(
        body,
        grid_spec=pltpu.PrefetchScalarGridSpec(
            num_scalar_prefetch=1,
            grid=(rows // block,),
            in_specs=[pl.BlockSpec((block, width), here), pl.BlockSpec((block, width), here)]
            + ([] if prev is None else [pl.BlockSpec(memory_space=pl.ANY)]),
            out_specs=pl.BlockSpec((block, width), lambda i, h: (i + row // block, h[0]))),
        out_shape=jax.ShapeDtypeStruct(shape, F32),
        input_output_aliases={} if prev is None else {3: 0},
        compiler_params=params(),
        cost_estimate=cost(rows * width, 12 * rows * width),
        name="total",
    )(half, a, b, *(() if prev is None else (prev,)))


def solution(mesh):
    dp_size = mesh.shape["dp"]
    swap_tp = [(0, 1), (1, 0)]
    swap_x = [(i, i ^ 2) for i in range(dp_size)]
    swap_core = [(i, i ^ 1) for i in range(dp_size)]

    def local_step(h_teacher, h_student, w_teacher, w_student):
        tokens, depth = h_student.shape
        tok_total = tokens * dp_size
        half = tokens // 2
        tp = lax.axis_index("tp")
        dp = lax.axis_index("dp")
        core, x = dp % 2, dp // 2
        both = (w_teacher, w_student)
        quarter, beside = 2 * core + x, 2 * core + 1 - x

        def over(axis, perm, v):
            return lax.ppermute(v, axis, perm)

        def to_tp(v):
            return over("tp", swap_tp, v)

        def to_x(v):
            return over("dp", swap_x, v)

        def to_core(v):
            return over("dp", swap_core, v)

        y0 = to_tp(cast_part(both, [quarter]))
        y1 = to_tp(cast_part(both, [4 + quarter]))
        et, es, stat_a = logits_part(h_teacher, h_student, w_teacher, w_student, 0, half, None)
        x0 = to_x(y0)
        et, es, stat_b = logits_part(h_teacher, h_student, w_teacher, w_student, half, half, (et, es))
        stat = jnp.concatenate([stat_a, stat_b], axis=1)
        stat_other = to_tp(stat)
        x1 = to_x(y1)

        first = jnp.where(tp == 0, stat, stat_other)
        second = jnp.where(tp == 0, stat_other, stat)
        max_t = jnp.maximum(first[0], second[0])
        max_s = jnp.maximum(first[2], second[2])
        scale_t1, scale_t2 = jnp.exp(first[0] - max_t), jnp.exp(second[0] - max_t)
        scale_s1, scale_s2 = jnp.exp(first[2] - max_s), jnp.exp(second[2] - max_s)
        sum_t = first[1] * scale_t1 + second[1] * scale_t2
        sum_s = first[3] * scale_s1 + second[3] * scale_s2
        inv_t = (1.0 / sum_t) / tok_total
        inv_s = (1.0 / sum_s) / tok_total
        own_t = jnp.exp(stat[0] - max_t) * inv_t
        own_s = jnp.exp(stat[2] - max_s) * inv_s
        num = (scale_t1 * (first[4] + first[1] * ((first[0] - max_t) - (first[2] - max_s)))
               + scale_t2 * (second[4] + second[1] * ((second[0] - max_t) - (second[2] - max_s))))
        kl = num / sum_t - (jnp.log(sum_t) - jnp.log(sum_s))
        coef = jnp.stack([own_t, own_s, max_t, inv_t, max_s, inv_s, kl, jnp.zeros_like(kl)])

        casts = (cast_part((w_student,), [8 + quarter]), cast_part((w_teacher,), [8 + quarter, 8 + beside]),
                 cast_part(both, [12 + core]), cast_part(both, [14 + core]))
        casts, coef = lax.optimization_barrier((casts, coef))
        y2s = to_tp(casts[0])
        y2t = to_tp(casts[1])
        y3 = to_tp(casts[2])
        y4 = to_tp(casts[3])
        core_at = jnp.reshape(core, (1,)).astype(jnp.int32)
        dh, mine, theirs = grads_part(core_at, h_student, w_student, et, es, coef)
        got = to_core(theirs)
        cy0, cx0 = to_core(y0), to_core(x0)
        cy1, cx1 = to_core(y1), to_core(x1)
        x2s = to_x(y2s)
        cy2s, cx2s, cy2t = to_core(y2s), to_core(x2s), to_core(y2t)
        cy3, cy4 = to_core(y3), to_core(y4)

        cut = depth // 2
        chip_a, chip_b = mine[0:cut] + got[0:cut], mine[cut:] + got[cut:]
        far_a, far_b = to_x(chip_a), to_x(chip_b)
        beside_a, beside_b = to_core(chip_a), to_core(chip_b)
        cross_a, cross_b = to_core(far_a), to_core(far_b)

        for pieces in ((("ts", y0), ("ts", x0), ("ts", cy0), ("ts", cx0)),
                             (("ts", y1), ("ts", x1), ("ts", cy1), ("ts", cx1)),
                             (("t", y2t), ("t", cy2t), ("s", y2s), ("s", x2s), ("s", cy2s), ("s", cx2s)),
                             (("ts", y3), ("ts", cy3)),
                             (("ts", y4), ("ts", cy4))):
            dh = other_part(h_teacher, h_student, coef, pieces, dh)

        shape = w_student.shape
        dw = total_part(core_at, chip_a, far_a, 0, cut, shape)
        dw = total_part(1 - core_at, beside_a, cross_a, 0, cut, shape, dw)
        dw = total_part(core_at, chip_b, far_b, cut, cut, shape, dw)
        dw = total_part(1 - core_at, beside_b, cross_b, cut, cut, shape, dw)
        kl_loss = jnp.sum(chip_b[cut + 6] + far_b[cut + 6]) / tok_total
        return kl_loss, dh, dw

    return jax.shard_map(
        local_step, mesh=mesh,
        in_specs=(P("dp", None), P("dp", None), P(None, "tp"), P(None, "tp")),
        out_specs=(P(), P("dp", None), P(None, "tp")),
        check_vma=False)
```

```python
import functools

import jax
import jax.numpy as jnp
from jax import lax
from jax.experimental import pallas as pl
from jax.experimental.pallas import tpu as pltpu
from jax.sharding import PartitionSpec as P

F32 = jnp.float32
BF16 = jnp.bfloat16
VMEM_LIMIT = 67043328
ONCE = pl.Buffered(buffer_count=1)


def params():
    return pltpu.CompilerParams(vmem_limit_bytes=VMEM_LIMIT, dimension_semantics=("arbitrary",))


def cost(flops, nbytes):
    return pl.CostEstimate(flops=int(flops), bytes_accessed=int(nbytes), transcendentals=0)


def lane_fold(x, op):
    acc = x[:, 0:128]
    for j in range(1, x.shape[1] // 128):
        acc = op(acc, x[:, 128 * j:128 * (j + 1)])
    return acc


def logits_body(rows, tile, ht_ref, hs_ref, wt_ref, ws_ref, *rest):
    et_ref, es_ref, stat_ref = rest[-3:]
    block, cols = et_ref.shape

    @pl.loop(0, block, step=rows)
    def _(r):
        sl = pl.ds(pl.multiple_of(r, rows), rows)
        ht = ht_ref[sl, :]
        hs = hs_ref[sl, :]
        mt = jnp.full((rows, 128), -jnp.inf, F32)
        ms = mt
        for c in range(0, cols, tile):
            zt = jnp.dot(ht, wt_ref[:, c:c + tile], preferred_element_type=F32)
            et_ref[sl, c:c + tile] = zt
            mt = jnp.maximum(mt, lane_fold(zt, jnp.maximum))
            zs = jnp.dot(hs, ws_ref[:, c:c + tile], preferred_element_type=F32)
            es_ref[sl, c:c + tile] = zs
            ms = jnp.maximum(ms, lane_fold(zs, jnp.maximum))
        mt = jnp.max(mt, axis=1, keepdims=True)
        ms = jnp.max(ms, axis=1, keepdims=True)
        st = jnp.zeros((rows, 128), F32)
        ss = st
        dd = st
        for c in range(0, cols, 128):
            xt = et_ref[sl, c:c + 128] - mt
            xs = es_ref[sl, c:c + 128] - ms
            pt = jnp.exp(xt)
            ps = jnp.exp(xs)
            et_ref[sl, c:c + 128] = pt
            es_ref[sl, c:c + 128] = ps
            st = st + pt
            ss = ss + ps
            dd = dd + pt * (xt - xs)
        vals = (mt, jnp.sum(st, axis=1, keepdims=True), ms, jnp.sum(ss, axis=1, keepdims=True),
                jnp.sum(dd, axis=1, keepdims=True))
        lane = lax.broadcasted_iota(jnp.int32, (rows, 128), 1)
        packed = jnp.zeros((rows, 128), F32)
        for i, v in enumerate(vals):
            packed = jnp.where(lane == i, v, packed)
        stat_ref[:, sl] = jnp.transpose(packed)[0:8, :]


def logits_part(ht, hs, wt, ws, start, count, prev, block=512, rows=256, tile=512):
    tokens, kt = ht.shape
    ks, cols = ws.shape
    first = start // block
    tok = lambda i: (i + first, 0)
    fixed = lambda i: (0, 0)
    in_specs = [pl.BlockSpec((block, kt), tok), pl.BlockSpec((block, ks), tok),
                pl.BlockSpec((kt, cols), fixed, pipeline_mode=ONCE),
                pl.BlockSpec((ks, cols), fixed, pipeline_mode=ONCE)]
    args = [ht, hs, wt, ws]
    alias = {}
    if prev is not None:
        in_specs += [pl.BlockSpec(memory_space=pl.ANY)] * 2
        args += list(prev)
        alias = {4: 0, 5: 1}
    return pl.pallas_call(
        functools.partial(logits_body, rows, tile),
        grid=(count // block,),
        in_specs=in_specs,
        out_specs=[pl.BlockSpec((block, cols), tok), pl.BlockSpec((block, cols), tok),
                   pl.BlockSpec((8, block), lambda i: (0, i))],
        out_shape=[jax.ShapeDtypeStruct((tokens, cols), F32), jax.ShapeDtypeStruct((tokens, cols), F32),
                   jax.ShapeDtypeStruct((8, count), F32)],
        input_output_aliases=alias,
        compiler_params=params(),
        cost_estimate=cost(2 * count * cols * (kt + ks), 2 * cols * (kt + ks) + count * (2 * (kt + ks) + 8 * cols)),
        name="logits",
    )(*args)


def grads_body(core_ref, hs_ref, ws_ref, et_ref, es_ref, coef_ref, dh_ref, mine_hbm, theirs_hbm, acc_ref, sem):
    i = pl.program_id(0)
    core = core_ref[0]
    block, ks = hs_ref.shape
    width = acc_ref.shape[2]

    @pl.when(i == 0)
    def _():
        acc_ref[...] = jnp.zeros(acc_ref.shape, F32)

    coef = jnp.transpose(coef_ref[...])
    dz = (es_ref[...] * coef[:, 1:2] - et_ref[...] * coef[:, 0:1]).astype(BF16)
    dh_ref[...] = lax.dot_general(dz, ws_ref[...], (((1,), (1,)), ((), ())), preferred_element_type=F32)
    hs_t = jnp.transpose(hs_ref[...])
    for c in range(0, 2 * width, 512):
        half, at = c // width, c % width
        acc_ref[half, 0:ks, at:at + 512] += jnp.dot(hs_t, dz[:, c:c + 512], preferred_element_type=F32)
    for half in range(2):
        acc_ref[half, ks:ks + 8, 0:block] += coef_ref[...]

    @pl.when(i == pl.num_programs(0) - 1)
    def _():
        first = pltpu.make_async_copy(acc_ref.at[1 - core], theirs_hbm, sem.at[0])
        second = pltpu.make_async_copy(acc_ref.at[core], mine_hbm, sem.at[1])
        first.start()
        second.start()
        first.wait()
        second.wait()


def grads_part(core, hs, ws, et, es, coef, block=512):
    tokens, ks = hs.shape
    cols = ws.shape[1]
    tok = lambda i, c: (i, 0)
    half = jax.ShapeDtypeStruct((ks + 8, cols // 2), F32)
    return pl.pallas_call(
        grads_body,
        grid_spec=pltpu.PrefetchScalarGridSpec(
            num_scalar_prefetch=1,
            grid=(tokens // block,),
            in_specs=[pl.BlockSpec((block, ks), tok), pl.BlockSpec((ks, cols), lambda i, c: (0, 0), pipeline_mode=ONCE),
                      pl.BlockSpec((block, cols), tok), pl.BlockSpec((block, cols), tok),
                      pl.BlockSpec((8, block), lambda i, c: (0, i))],
            out_specs=[pl.BlockSpec((block, ks), tok), pl.BlockSpec(memory_space=pl.ANY),
                       pl.BlockSpec(memory_space=pl.ANY)],
            scratch_shapes=[pltpu.VMEM((2, ks + 8, cols // 2), F32), pltpu.SemaphoreType.DMA((2,))]),
        out_shape=[jax.ShapeDtypeStruct((tokens, ks), F32), half, half],
        compiler_params=params(),
        cost_estimate=cost(4 * tokens * cols * ks, 2 * ks * cols + tokens * (6 * ks + 8 * cols) + 4 * ks * cols),
        name="grads",
    )(core, hs, ws, et, es, coef)


def other_body(kinds, rows, ht_ref, hs_ref, coef_ref, *rest):
    pieces = rest[:len(kinds)]
    dh_in_ref, dh_ref, wt_ref, ws_ref = rest[len(kinds):]
    kt = ht_ref.shape[1]

    @pl.when(pl.program_id(0) == 0)
    def _():
        at_t = at_s = 0
        for kind, p in zip(kinds, pieces):
            w = p.shape[1]
            if "t" in kind:
                wt_ref[:, at_t:at_t + w] = p[0:kt, :].astype(BF16)
                at_t += w
            if "s" in kind:
                ws_ref[:, at_s:at_s + w] = p[p.shape[0] - ws_ref.shape[0]:, :].astype(BF16)
                at_s += w

    for r in range(0, ht_ref.shape[0], rows):
        sl = pl.ds(r, rows)
        coef = jnp.transpose(coef_ref[:, r:r + rows])
        zt = jnp.dot(ht_ref[sl, :], wt_ref[...], preferred_element_type=F32)
        zs = jnp.dot(hs_ref[sl, :], ws_ref[...], preferred_element_type=F32)
        pt = jnp.exp(zt - coef[:, 2:3]) * coef[:, 3:4]
        ps = jnp.exp(zs - coef[:, 4:5]) * coef[:, 5:6]
        dz = (ps - pt).astype(BF16)
        dh_ref[sl, :] = dh_in_ref[sl, :] + lax.dot_general(
            dz, ws_ref[...], (((1,), (1,)), ((), ())), preferred_element_type=F32)


def other_part(ht, hs, coef, pieces, dh, block=512, rows=512):
    tokens, kt = ht.shape
    ks = hs.shape[1]
    kinds = tuple(k for k, _ in pieces)
    arrays = [p for _, p in pieces]
    cols = sum(p.shape[1] for k, p in pieces if "t" in k)
    tok = lambda i: (i, 0)
    fixed = lambda i: (0, 0)
    n = len(pieces)
    return pl.pallas_call(
        functools.partial(other_body, kinds, rows),
        grid=(tokens // block,),
        in_specs=[pl.BlockSpec((block, kt), tok), pl.BlockSpec((block, ks), tok), pl.BlockSpec((8, block), lambda i: (0, i))]
        + [pl.BlockSpec(p.shape, fixed, pipeline_mode=ONCE) for p in arrays]
        + [pl.BlockSpec((block, ks), tok)],
        out_specs=pl.BlockSpec((block, ks), tok),
        out_shape=jax.ShapeDtypeStruct((tokens, ks), F32),
        scratch_shapes=[pltpu.VMEM((kt, cols), BF16), pltpu.VMEM((ks, cols), BF16)],
        input_output_aliases={3 + n: 0},
        compiler_params=params(),
        cost_estimate=cost(2 * tokens * cols * (kt + 2 * ks), 4 * cols * (kt + ks) + tokens * (2 * kt + 10 * ks)),
        name="other",
    )(ht, hs, coef, *arrays, dh)


def cast_part(weights, blocks):
    depth = sum(w.shape[0] for w in weights)

    def body(at_ref, *refs):
        row = 0
        for ref in refs[:-1]:
            refs[-1][row:row + ref.shape[0], :] = ref[...].astype(F32)
            row += ref.shape[0]

    return pl.pallas_call(
        body,
        grid_spec=pltpu.PrefetchScalarGridSpec(
            num_scalar_prefetch=1,
            grid=(len(blocks),),
            in_specs=[pl.BlockSpec((w.shape[0], 128), lambda i, at: (0, at[i])) for w in weights],
            out_specs=pl.BlockSpec((depth, 128), lambda i, at: (0, i))),
        out_shape=jax.ShapeDtypeStruct((depth, 128 * len(blocks)), F32),
        compiler_params=params(),
        cost_estimate=cost(128 * depth, 768 * depth * len(blocks)),
        name="cast",
    )(jnp.stack(blocks).astype(jnp.int32), *weights)


def total_part(half, a, b, row, rows, shape, prev=None, block=384):
    width = shape[1] // 2

    def body(half_ref, a_ref, b_ref, *rest):
        rest[-1][...] = a_ref[...] + b_ref[...]

    here = lambda i, h: (i, 0)
    return pl.pallas_call(
        body,
        grid_spec=pltpu.PrefetchScalarGridSpec(
            num_scalar_prefetch=1,
            grid=(rows // block,),
            in_specs=[pl.BlockSpec((block, width), here), pl.BlockSpec((block, width), here)]
            + ([] if prev is None else [pl.BlockSpec(memory_space=pl.ANY)]),
            out_specs=pl.BlockSpec((block, width), lambda i, h: (i + row // block, h[0]))),
        out_shape=jax.ShapeDtypeStruct(shape, F32),
        input_output_aliases={} if prev is None else {3: 0},
        compiler_params=params(),
        cost_estimate=cost(rows * width, 12 * rows * width),
        name="total",
    )(half, a, b, *(() if prev is None else (prev,)))


def solution(mesh):
    dp_size = mesh.shape["dp"]
    swap_tp = [(0, 1), (1, 0)]
    swap_x = [(i, i ^ 2) for i in range(dp_size)]
    swap_core = [(i, i ^ 1) for i in range(dp_size)]

    def local_step(h_teacher, h_student, w_teacher, w_student):
        tokens, depth = h_student.shape
        tok_total = tokens * dp_size
        half = tokens // 2
        tp = lax.axis_index("tp")
        dp = lax.axis_index("dp")
        core, x = dp % 2, dp // 2
        both = (w_teacher, w_student)
        quarter, beside = 2 * core + x, 2 * core + 1 - x

        def over(axis, perm, v):
            return lax.ppermute(v, axis, perm)

        def to_tp(v):
            return over("tp", swap_tp, v)

        def to_x(v):
            return over("dp", swap_x, v)

        def to_core(v):
            return over("dp", swap_core, v)

        y0 = to_tp(cast_part(both, [quarter]))
        y1 = to_tp(cast_part(both, [4 + quarter]))
        et, es, stat_a = logits_part(h_teacher, h_student, w_teacher, w_student, 0, half, None)
        x0 = to_x(y0)
        et, es, stat_b = logits_part(h_teacher, h_student, w_teacher, w_student, half, half, (et, es))
        stat = jnp.concatenate([stat_a, stat_b], axis=1)
        stat_other = to_tp(stat)
        x1 = to_x(y1)

        first = jnp.where(tp == 0, stat, stat_other)
        second = jnp.where(tp == 0, stat_other, stat)
        max_t = jnp.maximum(first[0], second[0])
        max_s = jnp.maximum(first[2], second[2])
        scale_t1, scale_t2 = jnp.exp(first[0] - max_t), jnp.exp(second[0] - max_t)
        scale_s1, scale_s2 = jnp.exp(first[2] - max_s), jnp.exp(second[2] - max_s)
        sum_t = first[1] * scale_t1 + second[1] * scale_t2
        sum_s = first[3] * scale_s1 + second[3] * scale_s2
        inv_t = (1.0 / sum_t) / tok_total
        inv_s = (1.0 / sum_s) / tok_total
        own_t = jnp.exp(stat[0] - max_t) * inv_t
        own_s = jnp.exp(stat[2] - max_s) * inv_s
        num = (scale_t1 * (first[4] + first[1] * ((first[0] - max_t) - (first[2] - max_s)))
               + scale_t2 * (second[4] + second[1] * ((second[0] - max_t) - (second[2] - max_s))))
        kl = num / sum_t - (jnp.log(sum_t) - jnp.log(sum_s))
        coef = jnp.stack([own_t, own_s, max_t, inv_t, max_s, inv_s, kl, jnp.zeros_like(kl)])

        casts = (cast_part((w_student,), [8 + quarter]), cast_part((w_teacher,), [8 + quarter, 8 + beside]),
                 cast_part(both, [12 + core]), cast_part(both, [14 + core]))
        casts, coef = lax.optimization_barrier((casts, coef))
        y2s = to_tp(casts[0])
        y2t = to_tp(casts[1])
        y3 = to_tp(casts[2])
        y4 = to_tp(casts[3])
        core_at = jnp.reshape(core, (1,)).astype(jnp.int32)
        dh, mine, theirs = grads_part(core_at, h_student, w_student, et, es, coef)
        got = to_core(theirs)
        cy0, cx0 = to_core(y0), to_core(x0)
        cy1, cx1 = to_core(y1), to_core(x1)
        x2s = to_x(y2s)
        cy2s, cx2s, cy2t = to_core(y2s), to_core(x2s), to_core(y2t)
        cy3, cy4 = to_core(y3), to_core(y4)

        cut = depth // 2
        chip_a, chip_b = mine[0:cut] + got[0:cut], mine[cut:] + got[cut:]
        far_a, far_b = to_x(chip_a), to_x(chip_b)
        beside_a, beside_b = to_core(chip_a), to_core(chip_b)
        cross_a, cross_b = to_core(far_a), to_core(far_b)

        for pieces in ((("ts", y0), ("ts", x0), ("ts", cy0), ("ts", cx0),
                                     ("ts", y1), ("ts", x1), ("ts", cy1), ("ts", cx1)),
                             (("t", y2t), ("t", cy2t), ("s", y2s), ("s", x2s), ("s", cy2s), ("s", cx2s)),
                             (("ts", y3), ("ts", cy3), ("ts", y4), ("ts", cy4))):
            dh = other_part(h_teacher, h_student, coef, pieces, dh)

        shape = w_student.shape
        dw = total_part(core_at, chip_a, far_a, 0, cut, shape)
        dw = total_part(1 - core_at, beside_a, cross_a, 0, cut, shape, dw)
        dw = total_part(core_at, chip_b, far_b, cut, cut, shape, dw)
        dw = total_part(1 - core_at, beside_b, cross_b, cut, cut, shape, dw)
        kl_loss = jnp.sum(chip_b[cut + 6] + far_b[cut + 6]) / tok_total
        return kl_loss, dh, dw

    return jax.shard_map(
        local_step, mesh=mesh,
        in_specs=(P("dp", None), P("dp", None), P(None, "tp"), P(None, "tp")),
        out_specs=(P(), P("dp", None), P(None, "tp")),
        check_vma=False)
```
